32 devices in a mesh: dp: 4 (over y, z), tp: 8 (over x, core).
Axes of the slice: x: 4, y: 2, z: 2, core: 2. Of those that a mesh axis runs over, the one named last changes fastest.
The devices are a block of a 4x4x8 slice.
Arguments:
- hidden: bfloat16 [64, 256, 2560], P('dp', 'tp'), parts along dimension 0
- norm_gain: bfloat16 [2560], replicated
- w_dq: bfloat16 [2560, 768], replicated
- q_gain: bfloat16 [768], replicated
- w_dkv: bfloat16 [2560, 288], replicated
- kv_gain: bfloat16 [256], replicated
- w_uq: bfloat16 [768, 128, 64], P(None, 'tp')
- w_qr: bfloat16 [768, 128, 32], P(None, 'tp')
- w_uk: bfloat16 [256, 128, 64], P(None, 'tp')
- w_uv: bfloat16 [256, 128, 64], P(None, 'tp')
- w_out: bfloat16 [128, 64, 2560], P('tp')
- rope_cos: float32 [256, 16], replicated
- rope_sin: float32 [256, 16], replicated
- grad_out: bfloat16 [64, 256, 2560], P('dp', 'tp'), parts along dimension 0
Outputs:
- output 1: bfloat16 [64, 256, 2560], P('dp', 'tp'), parts along dimension 0
- output 2: float32 [64, 256, 2560], P('dp', 'tp'), parts along dimension 0
- output 3: float32 [10240], P('dp'), parts along dimension 0
- output 4: float32 [10240, 768], P('dp'), parts along dimension 0
- output 5: float32 [3072], P('dp'), parts along dimension 0
- output 6: float32 [10240, 288], P('dp'), parts along dimension 0
- output 7: float32 [1024], P('dp'), parts along dimension 0
- output 8: float32 [3072, 128, 64], P('dp', 'tp'), parts along dimension 0
- output 9: float32 [3072, 128, 32], P('dp', 'tp'), parts along dimension 0
- output 10: float32 [1024, 128, 64], P('dp', 'tp'), parts along dimension 0
- output 11: float32 [1024, 128, 64], P('dp', 'tp'), parts along dimension 0
- output 12: float32 [512, 64, 2560], P(('dp', 'tp')), parts along dimension 0
There are 4 independent parts. The reference program is written for one: setup_inputs(seed, part) draws one part's arguments, and reference() takes and returns one part's arrays. A program takes and returns all parts, laid end to end along the dimension named above; an argument that names none is the same for every part.
All inputs are finite; a program needn't handle non-finite values.
Results may differ from the reference program's by a relative error of at most 0.0171253.
Values are sent between devices in bfloat16 or wider.
A program may use at most 768 MiB of HBM per device.

```python
import jax
import jax.numpy as jnp
from jax import lax

BATCH_SIZE = 16
SEQ_LEN = 256
MODEL_DIM = 2560
NUM_HEADS = 128
Q_RANK = 768
KV_RANK = 256
NOPE_DIM = 64
ROPE_DIM = 32
VALUE_DIM = 64
NORM_EPS = 1e-6


def setup_inputs(seed: int = 0, part: int = 0) -> dict:
    base_key = jax.random.key(seed)
    part_keys = jax.random.split(jax.random.fold_in(base_key, part), 3)
    shared_keys = jax.random.split(base_key, 12)
    act_shape = (BATCH_SIZE, SEQ_LEN, MODEL_DIM)
    mean_row = jax.random.normal(part_keys[0], (1, 1, MODEL_DIM), jnp.float32)
    hidden = 0.8 * mean_row + jax.random.normal(part_keys[1], act_shape, jnp.float32)
    grad_out = jax.random.normal(part_keys[2], act_shape, jnp.float32)

    def make_gain(key, width):
        return (1.0 + 0.4 * jax.random.normal(key, (width,), jnp.float32)).astype(jnp.bfloat16)

    def make_dense(key, shape, fan_in):
        return (jax.random.normal(key, shape, jnp.float32) * fan_in ** -0.5).astype(jnp.bfloat16)

    step_gaps = jax.random.randint(shared_keys[11], (SEQ_LEN,), 1, 4)
    positions = jnp.cumsum(step_gaps).astype(jnp.float32)
    inv_freq = 10000.0 ** (-jnp.arange(ROPE_DIM // 2, dtype=jnp.float32) * 2.0 / ROPE_DIM)
    angles = positions[:, None] * inv_freq[None, :]
    return {
        'hidden': hidden.astype(jnp.bfloat16),
        'norm_gain': make_gain(shared_keys[0], MODEL_DIM),
        'w_dq': make_dense(shared_keys[1], (MODEL_DIM, Q_RANK), MODEL_DIM),
        'q_gain': make_gain(shared_keys[2], Q_RANK),
        'w_dkv': make_dense(shared_keys[3], (MODEL_DIM, KV_RANK + ROPE_DIM), MODEL_DIM),
        'kv_gain': make_gain(shared_keys[4], KV_RANK),
        'w_uq': make_dense(shared_keys[5], (Q_RANK, NUM_HEADS, NOPE_DIM), Q_RANK),
        'w_qr': make_dense(shared_keys[6], (Q_RANK, NUM_HEADS, ROPE_DIM), Q_RANK),
        'w_uk': make_dense(shared_keys[7], (KV_RANK, NUM_HEADS, NOPE_DIM), KV_RANK),
        'w_uv': make_dense(shared_keys[8], (KV_RANK, NUM_HEADS, VALUE_DIM), KV_RANK),
        'w_out': make_dense(shared_keys[9], (NUM_HEADS, VALUE_DIM, MODEL_DIM), NUM_HEADS * VALUE_DIM),
        'rope_cos': jnp.cos(angles),
        'rope_sin': jnp.sin(angles),
        'grad_out': grad_out.astype(jnp.bfloat16),
    }


def to_bf16(value):
    return value.astype(jnp.bfloat16).astype(jnp.float32)


def rms_norm(value, gain_vec):
    mean_sq = jnp.mean(value * value, axis=-1, keepdims=True)
    return value * lax.rsqrt(mean_sq + NORM_EPS) * gain_vec


def apply_rope(value, cos_tab, sin_tab):
    half_dim = value.shape[-1] // 2
    lead_half = value[..., :half_dim]
    tail_half = value[..., half_dim:]
    return jnp.concatenate([lead_half * cos_tab - tail_half * sin_tab, tail_half * cos_tab + lead_half * sin_tab], axis=-1)


def block_forward(hidden, norm_gain, w_dq, q_gain, w_dkv, kv_gain, w_uq, w_qr, w_uk, w_uv, w_out, rope_cos, rope_sin):
    normed = to_bf16(rms_norm(hidden, norm_gain))
    q_latent = to_bf16(jnp.einsum('bsd,dr->bsr', normed, w_dq, preferred_element_type=jnp.float32))
    q_normed = to_bf16(rms_norm(q_latent, q_gain))
    q_nope = to_bf16(jnp.einsum('bsr,rhn->hbsn', q_normed, w_uq, preferred_element_type=jnp.float32))
    q_rope_in = to_bf16(jnp.einsum('bsr,rhn->hbsn', q_normed, w_qr, preferred_element_type=jnp.float32))
    q_rope = to_bf16(apply_rope(q_rope_in, rope_cos, rope_sin))
    kv_latent = to_bf16(jnp.einsum('bsd,dr->bsr', normed, w_dkv, preferred_element_type=jnp.float32))
    kv_normed = to_bf16(rms_norm(kv_latent[..., :KV_RANK], kv_gain))
    k_rope = to_bf16(apply_rope(kv_latent[..., KV_RANK:], rope_cos, rope_sin))
    k_nope = to_bf16(jnp.einsum('bsr,rhn->hbsn', kv_normed, w_uk, preferred_element_type=jnp.float32))
    values = to_bf16(jnp.einsum('bsr,rhv->hbsv', kv_normed, w_uv, preferred_element_type=jnp.float32))
    causal = jnp.arange(SEQ_LEN)[:, None] >= jnp.arange(SEQ_LEN)[None, :]
    score_scale = (NOPE_DIM + ROPE_DIM) ** -0.5

    def head_attention(operands):
        q_nope_h, q_rope_h, k_nope_h, value_h = operands
        scores = (jnp.einsum('bqn,bkn->bqk', q_nope_h, k_nope_h) + jnp.einsum('bqr,bkr->bqk', q_rope_h, k_rope)) * score_scale
        scores = jnp.where(causal, scores, -1e30)
        attn_prob = to_bf16(jax.nn.softmax(scores, axis=-1))
        return to_bf16(jnp.einsum('bqk,bkv->bqv', attn_prob, value_h))

    head_out = lax.map(jax.checkpoint(head_attention), (q_nope, q_rope, k_nope, values))
    attn_out = to_bf16(jnp.einsum('hbsv,hvd->bsd', head_out, w_out, preferred_element_type=jnp.float32))
    return to_bf16(hidden + attn_out)


def reference(hidden, norm_gain, w_dq, q_gain, w_dkv, kv_gain, w_uq, w_qr, w_uk, w_uv, w_out, rope_cos, rope_sin, grad_out):
    primals = (hidden.astype(jnp.float32), norm_gain.astype(jnp.float32), w_dq.astype(jnp.float32), q_gain.astype(jnp.float32), w_dkv.astype(jnp.float32), kv_gain.astype(jnp.float32), w_uq.astype(jnp.float32), w_qr.astype(jnp.float32), w_uk.astype(jnp.float32), w_uv.astype(jnp.float32), w_out.astype(jnp.float32))
    out_hidden, pullback = jax.vjp(lambda *params: block_forward(*params, rope_cos, rope_sin), *primals)
    grads = pullback(grad_out.astype(jnp.float32))
    return (out_hidden.astype(jnp.bfloat16), grads[0], grads[1], grads[2], grads[3], grads[4], grads[5], grads[6], grads[7], grads[8], grads[9], grads[10])
```

```python
import functools

import jax
import jax.numpy as jnp
from jax import lax
from jax.experimental import pallas as pl
from jax.experimental.pallas import tpu as pltpu
from jax.sharding import PartitionSpec as P


NORM_EPS = 1e-6
LOG2_E = 1.4426950408889634
MASKED = -1e30
FORWARD_AHEAD = 4
BACKWARD_AHEAD = 2
F32 = jnp.float32
BF16 = jnp.bfloat16


def norm_forward(value, gain_vec):
    value32 = value.astype(F32)
    inv_rms = lax.rsqrt(jnp.mean(value32 * value32, axis=-1, keepdims=True) + NORM_EPS)
    unit_val = value32 * inv_rms
    return (unit_val * gain_vec.astype(F32)).astype(BF16), unit_val, inv_rms


def norm_backward(grad_norm, unit_val, inv_rms, gain_vec):
    grad_unit = grad_norm * gain_vec.astype(F32)
    grad_in = inv_rms * (grad_unit - unit_val * jnp.mean(grad_unit * unit_val, axis=-1, keepdims=True))
    grad_gain = jnp.sum(grad_norm * unit_val, axis=tuple(range(grad_norm.ndim - 1)))
    return grad_in, grad_gain


def dot(lhs, rhs, lhs_dim, rhs_dim):
    return lax.dot_general(lhs, rhs, (((lhs_dim,), (rhs_dim,)), ((), ())), preferred_element_type=F32)


def whole(early, cross, late, half):
    blank = jnp.zeros((half, half), BF16)
    return jnp.concatenate([jnp.concatenate([early, cross], axis=1), jnp.concatenate([blank, late], axis=1)], axis=0)


def fill_slot(nope, rotary, side):
    blank = jnp.zeros((128 - nope.shape[0] - rotary.shape[0], nope.shape[1]), nope.dtype)
    parts = [nope, rotary, blank] if side == 0 else [rotary, blank, nope]
    return jnp.concatenate(parts, axis=0)


def forward_kernel(dims, score_scale, unroll, lat_ref, wq_ref, wk_ref, wv_ref, wo_ref, cos_ref, sin_ref, q_ref, o_ref, lse_ref, part_ref, k_buf, v_buf):
    q_rank, kv_rank, nope, rope, value = dims
    shards, _, rows, _ = lat_ref.shape
    seq = shards * rows
    half = seq // 2
    head = nope + rope
    mid = rope // 2
    pairs = wk_ref.shape[0] // (2 * nope)
    low = lax.broadcasted_iota(jnp.int32, (seq, 128), 1) < 64
    seen = lax.broadcasted_iota(jnp.int32, (half, half), 0) <= lax.broadcasted_iota(jnp.int32, (half, half), 1)
    key_scale = score_scale * LOG2_E
    q_lat = lat_ref[:, 0, :, :q_rank].reshape(seq, q_rank)
    kv_lat = lat_ref[:, 0, :, q_rank:q_rank + kv_rank].reshape(seq, kv_rank)
    k_rope = lat_ref[:, 0, :, q_rank + kv_rank:].reshape(seq, 128)
    half_q = wq_ref.shape[0] // 2

    def q_step(i, carry):
        at = pl.ds(pl.multiple_of(i * half_q, half_q), half_q)
        q_ref[0, at, :] = dot(wq_ref[at, :], q_lat, 1, 1).astype(BF16)
        return carry

    lax.fori_loop(0, 2, q_step, 0)
    k_buf[...] = dot(kv_lat, wk_ref[...], 1, 1).astype(BF16)
    v_buf[...] = dot(wv_ref[...], kv_lat, 1, 1).astype(BF16)
    cos, sin = cos_ref[...], sin_ref[...]

    def scores(h, side):
        at = h * head
        k_pair = k_buf[:, pl.ds((h - side) * 64, 128)]
        q_nope = q_ref[0, pl.ds(at, nope), :]
        tail = q_ref[0, pl.ds(at + nope, rope), :].astype(F32)
        lead, last = tail[:mid], tail[mid:]
        rotary = jnp.concatenate([lead * cos - last * sin, last * cos + lead * sin], axis=0).astype(BF16)
        q_ref[0, pl.ds(at + nope, rope), :] = rotary
        k = jnp.where(low, k_pair, k_rope) if side == 0 else jnp.where(low, k_rope, k_pair)
        return dot(k, fill_slot(q_nope, rotary, side), 1, 0)

    def attend(h, s):
        early = jnp.where(seen, s[:half, :half], MASKED)
        cross = s[:half, half:]
        late = jnp.where(seen, s[half:, half:], MASKED)
        peak0 = jnp.max(early, axis=0, keepdims=True)
        peak1 = jnp.maximum(jnp.max(cross, axis=0, keepdims=True), jnp.max(late, axis=0, keepdims=True))
        early = jnp.exp2((early - peak0) * key_scale)
        cross = jnp.exp2((cross - peak1) * key_scale)
        late = jnp.exp2((late - peak1) * key_scale)
        total0 = jnp.sum(early, axis=0, keepdims=True)
        total1 = jnp.sum(cross, axis=0, keepdims=True) + jnp.sum(late, axis=0, keepdims=True)
        inv0, inv1 = 1.0 / total0, 1.0 / total1
        prob = whole((early * inv0).astype(BF16), (cross * inv1).astype(BF16), (late * inv1).astype(BF16), half)
        peak = jnp.concatenate([peak0, peak1], axis=1)
        total = jnp.concatenate([total0, total1], axis=1)
        lse_ref[0, pl.ds(h, 1), :] = peak * key_scale + jnp.log2(total)
        return dot(v_buf[pl.ds(h * value, value), :], prob, 1, 0)

    def emit(pair, outs):
        o_pair = jnp.transpose(jnp.concatenate(outs, axis=0)).astype(BF16)
        o_ref[:, 0, :, pl.ds(pair * 128, 128)] = o_pair.reshape(shards, rows, 128)

    def group_step(i, carry):
        first = i * unroll * 2
        count = unroll * 2
        tiles = [scores(first + j, j % 2) if j < FORWARD_AHEAD else None for j in range(count)]
        outs = [None] * count
        for j in range(count):
            if j + FORWARD_AHEAD < count:
                tiles[j + FORWARD_AHEAD] = scores(first + j + FORWARD_AHEAD, (j + FORWARD_AHEAD) % 2)
            outs[j] = attend(first + j, tiles[j])
            if j % 2 == 1:
                emit(i * unroll + j // 2, outs[j - 1:j + 1])
        return carry

    if unroll == pairs:
        group_step(0, 0)
    else:
        lax.fori_loop(0, pairs // unroll, group_step, 0)
    o_all = o_ref[:, 0].reshape(seq, pairs * 2 * value)
    step = 512

    def out_step(i, carry):
        cols = pl.ds(pl.multiple_of(i * step, step), step)
        part_ref[:, 0, :, cols] = dot(o_all, wo_ref[:, cols], 1, 0).astype(BF16).reshape(shards, rows, step)
        return carry

    lax.fori_loop(0, part_ref.shape[3] // step, out_step, 0)


def backward_kernel(dims, score_scale, unroll, lat_ref, dy_ref, q_ref, lse_ref, wq_ref, wk_ref, wv_ref, wo_ref, cos_ref, sin_ref, glat_ref, gwq_ref, gwk_ref, gwv_ref, do_buf, dq_buf, dk_buf, dv_buf, rope_acc, k_buf, kt_buf, v_buf):
    q_rank, kv_rank, nope, rope, value = dims
    shards, _, rows, _ = lat_ref.shape
    seq = shards * rows
    half = seq // 2
    head = nope + rope
    mid = rope // 2
    pairs = wk_ref.shape[0] // (2 * nope)
    low = lax.broadcasted_iota(jnp.int32, (seq, 128), 1) < 64
    seen = lax.broadcasted_iota(jnp.int32, (half, half), 0) <= lax.broadcasted_iota(jnp.int32, (half, half), 1)
    key_scale = score_scale * LOG2_E
    q_lat = lat_ref[:, 0, :, :q_rank].reshape(seq, q_rank)
    kv_lat = lat_ref[:, 0, :, q_rank:q_rank + kv_rank].reshape(seq, kv_rank)
    k_rope = lat_ref[:, 0, :, q_rank + kv_rank:].reshape(seq, 128)
    k_rope_t = jnp.transpose(k_rope.astype(F32))[:rope].astype(BF16)
    dy = dy_ref[:, 0].reshape(seq, dy_ref.shape[3])
    step = 256

    def grad_out_step(i, carry):
        at = pl.ds(pl.multiple_of(i * step, step), step)
        do_buf[at, :] = dot(wo_ref[at, :], dy, 1, 1).astype(BF16)
        return carry

    lax.fori_loop(0, do_buf.shape[0] // step, grad_out_step, 0)
    k_buf[...] = dot(kv_lat, wk_ref[...], 1, 1).astype(BF16)
    kt_buf[...] = dot(wk_ref[...], kv_lat, 1, 1).astype(BF16)
    v_buf[...] = dot(kv_lat, wv_ref[...], 1, 1).astype(BF16)
    rope_acc[...] = jnp.zeros_like(rope_acc)
    cos, sin = cos_ref[...], sin_ref[...]
    none = jnp.zeros((value, seq), BF16)

    def scores(h, side):
        lanes = pl.ds((h - side) * 64, 128)
        q = q_ref[0, pl.ds(h * head, head), :]
        k_pair = k_buf[:, lanes]
        k = jnp.where(low, k_pair, k_rope) if side == 0 else jnp.where(low, k_rope, k_pair)
        do = do_buf[pl.ds(h * value, value), :]
        do_slot = jnp.concatenate([do, none] if side == 0 else [none, do], axis=0)
        s = dot(k, fill_slot(q[:nope], q[nope:], side), 1, 0)
        return s, dot(v_buf[:, lanes], do_slot, 1, 0)

    def finish(h, tiles):
        s, dp = tiles
        lse = lse_ref[0, pl.ds(h, 1), :]
        p_early = jnp.exp2(jnp.where(seen, s[:half, :half], MASKED) * key_scale - lse[:, :half])
        p_cross = jnp.exp2(s[:half, half:] * key_scale - lse[:, half:])
        p_late = jnp.exp2(jnp.where(seen, s[half:, half:], MASKED) * key_scale - lse[:, half:])
        prob = whole(p_early.astype(BF16), p_cross.astype(BF16), p_late.astype(BF16), half)
        dp_early, dp_cross, dp_late = dp[:half, :half], dp[:half, half:], dp[half:, half:]
        sum0 = jnp.sum(p_early * dp_early, axis=0, keepdims=True)
        sum1 = jnp.sum(p_cross * dp_cross, axis=0, keepdims=True) + jnp.sum(p_late * dp_late, axis=0, keepdims=True)
        ds_early = (p_early * (dp_early - sum0) * score_scale).astype(BF16)
        ds_cross = (p_cross * (dp_cross - sum1) * score_scale).astype(BF16)
        ds_late = (p_late * (dp_late - sum1) * score_scale).astype(BF16)
        return prob, whole(ds_early, ds_cross, ds_late, half)

    def products(h, prob, ds):
        rows64 = pl.ds(h * 64, 64)
        grad_v = dot(do_buf[rows64, :], prob, 1, 1)
        dv_buf[rows64, :] = grad_v.astype(BF16)
        grad_k = dot(q_ref[0, pl.ds(h * head, head), :], ds, 1, 1)
        k_t = jnp.concatenate([kt_buf[rows64, :], k_rope_t], axis=0)
        grad_q = dot(k_t, ds, 1, 0)
        lead, last = grad_q[nope:nope + mid], grad_q[nope + mid:]
        dq_buf[pl.ds(h * head, head), :] = jnp.concatenate([grad_q[:nope], lead * cos + last * sin, last * cos - lead * sin], axis=0).astype(BF16)
        dk_buf[rows64, :] = grad_k[:nope].astype(BF16)
        rope_acc[...] += grad_k[nope:]

    def group_step(i, carry):
        count = unroll * 2
        first = i * count
        tiles = [scores(first + j, j % 2) if j < BACKWARD_AHEAD else None for j in range(count)]
        held = None
        for j in range(count):
            if j + BACKWARD_AHEAD < count:
                tiles[j + BACKWARD_AHEAD] = scores(first + j + BACKWARD_AHEAD, (j + BACKWARD_AHEAD) % 2)
            done = finish(first + j, tiles[j])
            if held is not None:
                products(first + j - 1, *held)
            held = done
        products(first + count - 1, *held)
        return carry

    if unroll == pairs:
        group_step(0, 0)
    else:
        lax.fori_loop(0, pairs // unroll, group_step, 0)
    dq, dk, dv = dq_buf[...], dk_buf[...], dv_buf[...]
    glat_ref[:, 0, :, :q_rank] = dot(dq, wq_ref[...], 0, 0).astype(BF16).reshape(shards, rows, q_rank)
    grad_kv = dot(dk, wk_ref[...], 0, 0) + dot(dv, wv_ref[...], 0, 0)
    glat_ref[:, 0, :, q_rank:q_rank + kv_rank] = grad_kv.astype(BF16).reshape(shards, rows, kv_rank)
    padded = jnp.concatenate([rope_acc[...], jnp.zeros((128 - rope, seq), F32)], axis=0)
    glat_ref[:, 0, :, q_rank + kv_rank:] = jnp.transpose(padded).astype(BF16).reshape(shards, rows, 128)

    @pl.when(pl.program_id(0) == 0)
    def _():
        gwq_ref[...] = jnp.zeros_like(gwq_ref)
        gwk_ref[...] = jnp.zeros_like(gwk_ref)
        gwv_ref[...] = jnp.zeros_like(gwv_ref)

    def weight_step(i, carry):
        at = pl.ds(pl.multiple_of(i * step, step), step)
        gwq_ref[at, :] += dot(dq_buf[at, :], q_lat, 1, 0)
        return carry

    lax.fori_loop(0, dq_buf.shape[0] // step, weight_step, 0)
    gwk_ref[...] += dot(dk, kv_lat, 1, 0)
    gwv_ref[...] += dot(dv, kv_lat, 1, 0)


def solution(mesh):
    act_spec = P('dp', 'tp', None)
    head_spec = P(None, 'tp', None)
    in_specs = (act_spec, P(None), P(None, None), P(None), P(None, None), P(None), head_spec, head_spec, head_spec, head_spec, P('tp', None, None), P(None, None), P(None, None), act_spec)
    grad_head_spec = P('dp', 'tp', None)
    out_specs = (act_spec, act_spec, P('dp'), P('dp', None), P('dp'), P('dp', None), P('dp'), grad_head_spec, grad_head_spec, grad_head_spec, grad_head_spec, P(('dp', 'tp'), None, None))

    def local_step(hidden, norm_gain, w_dq, q_gain, w_dkv, kv_gain, w_uq, w_qr, w_uk, w_uv, w_out, rope_cos, rope_sin, grad_out):
        shards = mesh.shape['tp']
        batch, rows, dim = hidden.shape
        q_rank, kv_rank = q_gain.shape[0], kv_gain.shape[0]
        heads, nope = w_uq.shape[1:]
        rope = w_qr.shape[2]
        mid = rope // 2
        value = w_uv.shape[2]
        seq = shards * rows
        tokens = batch * seq
        here = batch * rows
        lat_width = q_rank + kv_rank + 128
        kv_width = kv_rank + rope
        score_scale = (nope + rope) ** -0.5

        x2 = hidden.reshape(here, dim)
        normed, x_unit, x_inv = norm_forward(x2, norm_gain)
        q_latent = dot(normed, w_dq, 1, 0).astype(BF16)
        kv_latent = dot(normed, w_dkv, 1, 0).astype(BF16)
        q_normed, q_unit, q_inv = norm_forward(q_latent, q_gain)
        kv_normed, kv_unit, kv_inv = norm_forward(kv_latent[:, :kv_rank], kv_gain)
        place = lax.axis_index('tp') * rows
        cos_here = jnp.tile(lax.dynamic_slice_in_dim(rope_cos, place, rows, 0), (batch, 1))
        sin_here = jnp.tile(lax.dynamic_slice_in_dim(rope_sin, place, rows, 0), (batch, 1))
        k_in = kv_latent[:, kv_rank:].astype(F32)
        k_lead, k_tail = k_in[:, :mid], k_in[:, mid:]
        k_rot = jnp.concatenate([k_lead * cos_here - k_tail * sin_here, k_tail * cos_here + k_lead * sin_here], axis=1).astype(BF16)
        k_none = jnp.zeros((here, 64 - rope), BF16)
        lat_here = jnp.concatenate([q_normed, kv_normed, k_rot, k_none, k_rot, k_none], axis=1).reshape(batch, rows, lat_width)
        lat_all = lax.all_gather(lat_here, 'tp', axis=0)
        dy_all = lax.all_gather(grad_out, 'tp', axis=0)

        wq = jnp.concatenate([w_uq.transpose(1, 2, 0), w_qr.transpose(1, 2, 0)], axis=1).reshape(heads * (nope + rope), q_rank)
        wk = w_uk.transpose(1, 2, 0).reshape(heads * nope, kv_rank)
        wv = w_uv.transpose(1, 2, 0).reshape(heads * value, kv_rank)
        w_o = w_out.reshape(heads * value, dim)
        weights = (wq, wk, wv, w_o, rope_cos.T, rope_sin.T)
        dims = (q_rank, kv_rank, nope, rope, value)

        def tok(width):
            return pl.BlockSpec((shards, 1, rows, width), lambda b: (0, b, 0, 0))

        def fixed(shape):
            return pl.BlockSpec(shape, lambda b: (0,) * len(shape))

        def per_batch(shape):
            return pl.BlockSpec((1,) + shape, lambda b: (b,) + (0,) * len(shape))

        def out(width):
            return jax.ShapeDtypeStruct((shards, batch, rows, width), BF16)

        weight_specs = [fixed(w.shape) for w in weights]
        attn_flops = 2 * batch * heads * seq * seq * 256
        up_flops = 2 * tokens * heads * ((nope + rope) * q_rank + (nope + value) * kv_rank)
        out_flops = 2 * tokens * heads * value * dim
        q_all, o_all, lse_all, attn_part = pl.pallas_call(
            functools.partial(forward_kernel, dims, score_scale, heads // 2),
            grid=(batch,),
            in_specs=[tok(lat_width)] + weight_specs,
            out_specs=[per_batch((wq.shape[0], seq)), tok(heads * value), per_batch((heads, seq)), tok(dim)],
            out_shape=[jax.ShapeDtypeStruct((batch, wq.shape[0], seq), BF16), out(heads * value), jax.ShapeDtypeStruct((batch, heads, seq), F32), out(dim)],
            scratch_shapes=[pltpu.VMEM((seq, heads * nope), BF16), pltpu.VMEM((heads * value, seq), BF16)],
            compiler_params=pltpu.CompilerParams(dimension_semantics=("arbitrary",)),
            cost_estimate=pl.CostEstimate(flops=attn_flops + up_flops + out_flops, bytes_accessed=70_000_000, transcendentals=batch * heads * seq * seq),
            name="attn_forward",
        )(lat_all, *weights)
        attn_out = lax.psum_scatter(attn_part, 'tp', scatter_dimension=0, tiled=False)
        out_hidden = (hidden.astype(F32) + attn_out.astype(F32)).astype(BF16)

        glat, gwq, gwk, gwv = pl.pallas_call(
            functools.partial(backward_kernel, dims, score_scale, heads // 2),
            grid=(batch,),
            in_specs=[tok(lat_width), tok(dim), per_batch((wq.shape[0], seq)), per_batch((heads, seq))] + weight_specs,
            out_specs=[tok(lat_width), fixed(wq.shape), fixed(wk.shape), fixed(wv.shape)],
            out_shape=[out(lat_width)] + [jax.ShapeDtypeStruct(w.shape, F32) for w in (wq, wk, wv)],
            scratch_shapes=[pltpu.VMEM((heads * value, seq), BF16), pltpu.VMEM((wq.shape[0], seq), BF16), pltpu.VMEM((heads * nope, seq), BF16), pltpu.VMEM((heads * value, seq), BF16), pltpu.VMEM((rope, seq), F32), pltpu.VMEM((seq, heads * nope), BF16), pltpu.VMEM((heads * nope, seq), BF16), pltpu.VMEM((seq, heads * value), BF16)],
            compiler_params=pltpu.CompilerParams(dimension_semantics=("arbitrary",)),
            cost_estimate=pl.CostEstimate(flops=3 * attn_flops + 3 * up_flops + out_flops, bytes_accessed=60_000_000, transcendentals=batch * heads * seq * seq),
            name="attn_backward",
        )(lat_all, dy_all, q_all, lse_all, *weights)
        grad_lat = lax.psum_scatter(glat, 'tp', scatter_dimension=0, tiled=False).reshape(here, lat_width).astype(F32)

        grad_wq = gwq.reshape(heads, nope + rope, q_rank)
        grad_w_uq = grad_wq[:, :nope].transpose(2, 0, 1)
        grad_w_qr = grad_wq[:, nope:].transpose(2, 0, 1)
        grad_w_uk = gwk.reshape(heads, nope, kv_rank).transpose(2, 0, 1)
        grad_w_uv = gwv.reshape(heads, value, kv_rank).transpose(2, 0, 1)
        grad_w_out = dot(o_all.reshape(tokens, heads * value), dy_all.reshape(tokens, dim), 0, 0).reshape(heads, value, dim)

        grad_q_lat, grad_q_gain = norm_backward(grad_lat[:, :q_rank], q_unit, q_inv, q_gain)
        grad_kv_lat, grad_kv_gain = norm_backward(grad_lat[:, q_rank:q_rank + kv_rank], kv_unit, kv_inv, kv_gain)
        gk = grad_lat[:, q_rank + kv_rank:q_rank + kv_rank + rope]
        gk_lead, gk_tail = gk[:, :mid], gk[:, mid:]
        grad_q_lat = grad_q_lat.astype(BF16)
        grad_kv_all = jnp.concatenate([grad_kv_lat, gk_lead * cos_here + gk_tail * sin_here, gk_tail * cos_here - gk_lead * sin_here], axis=1).astype(BF16)
        own = dim // shards
        own_kv = kv_width // shards * dim // q_rank
        part_dq = dot(normed, grad_q_lat, 0, 0).astype(BF16).reshape(shards, own, q_rank)
        part_dkv = dot(grad_kv_all, normed, 0, 0).astype(BF16).reshape(shards, own_kv, q_rank)
        down_sum = lax.psum_scatter(jnp.concatenate([part_dq, part_dkv], axis=1), 'tp', scatter_dimension=0, tiled=False)
        grad_normed = dot(grad_q_lat, w_dq, 1, 1) + dot(grad_kv_all, w_dkv, 1, 1)
        grad_x_norm, grad_norm_gain = norm_backward(grad_normed, x_unit, x_inv, norm_gain)
        grad_hidden = grad_out.reshape(here, dim).astype(F32) + grad_x_norm

        gains = jnp.concatenate([grad_norm_gain, grad_q_gain, grad_kv_gain])
        gain_rows = -(-gains.shape[0] // q_rank)
        gains = jnp.pad(gains, (0, gain_rows * q_rank - gains.shape[0])).reshape(gain_rows, q_rank)
        high = lax.reduce_precision(gains, 8, 7)
        middle = lax.reduce_precision(gains - high, 8, 7)
        tail = gains - high - middle
        packed = jnp.concatenate([down_sum, high.astype(BF16), middle.astype(BF16), tail.astype(BF16)], axis=0)
        gathered = lax.all_gather(packed, 'tp', axis=0)
        grad_w_dq = gathered[:, :own].reshape(dim, q_rank).astype(F32)
        grad_w_dkv = gathered[:, own:own + own_kv].reshape(kv_width, dim).astype(F32).T
        terms = gathered[:, own + own_kv:].astype(F32).reshape(shards, 3, gain_rows * q_rank)
        sums = jnp.sum(terms[:, 0] + terms[:, 1] + terms[:, 2], axis=0)
        g_norm = sums[:dim]
        g_q = sums[dim:dim + q_rank]
        g_kv = sums[dim + q_rank:dim + q_rank + kv_rank]
        return (out_hidden, grad_hidden.reshape(batch, rows, dim), g_norm, grad_w_dq, g_q, grad_w_dkv, g_kv, grad_w_uq, grad_w_qr, grad_w_uk, grad_w_uv, grad_w_out)

    return jax.shard_map(local_step, mesh=mesh, in_specs=in_specs, out_specs=out_specs, check_vma=False)
```

```python
import functools

import jax
import jax.numpy as jnp
from jax import lax
from jax.experimental import pallas as pl
from jax.experimental.pallas import tpu as pltpu
from jax.sharding import PartitionSpec as P


NORM_EPS = 1e-6
LOG2_E = 1.4426950408889634
MASKED = -1e30
FORWARD_AHEAD = 4
BACKWARD_AHEAD = 2
F32 = jnp.float32
BF16 = jnp.bfloat16


def norm_forward(value, gain_vec):
    value32 = value.astype(F32)
    inv_rms = lax.rsqrt(jnp.mean(value32 * value32, axis=-1, keepdims=True) + NORM_EPS)
    unit_val = value32 * inv_rms
    return (unit_val * gain_vec.astype(F32)).astype(BF16), unit_val, inv_rms


def norm_backward(grad_norm, unit_val, inv_rms, gain_vec):
    grad_unit = grad_norm * gain_vec.astype(F32)
    grad_in = inv_rms * (grad_unit - unit_val * jnp.mean(grad_unit * unit_val, axis=-1, keepdims=True))
    grad_gain = jnp.sum(grad_norm * unit_val, axis=tuple(range(grad_norm.ndim - 1)))
    return grad_in, grad_gain


def dot(lhs, rhs, lhs_dim, rhs_dim):
    return lax.dot_general(lhs, rhs, (((lhs_dim,), (rhs_dim,)), ((), ())), preferred_element_type=F32)


def whole(early, cross, late, half):
    blank = jnp.zeros((half, half), BF16)
    return jnp.concatenate([jnp.concatenate([early, cross], axis=1), jnp.concatenate([blank, late], axis=1)], axis=0)


def fill_slot(nope, rotary, side):
    blank = jnp.zeros((128 - nope.shape[0] - rotary.shape[0], nope.shape[1]), nope.dtype)
    parts = [nope, rotary, blank] if side == 0 else [rotary, blank, nope]
    return jnp.concatenate(parts, axis=0)


def forward_kernel(dims, score_scale, unroll, lat_ref, wq_ref, wk_ref, wv_ref, wo_ref, cos_ref, sin_ref, q_ref, o_ref, lse_ref, part_ref, k_buf, v_buf):
    q_rank, kv_rank, nope, rope, value = dims
    shards, _, rows, _ = lat_ref.shape
    seq = shards * rows
    half = seq // 2
    head = nope + rope
    mid = rope // 2
    pairs = wk_ref.shape[0] // (2 * nope)
    low = lax.broadcasted_iota(jnp.int32, (seq, 128), 1) < 64
    seen = lax.broadcasted_iota(jnp.int32, (half, half), 0) <= lax.broadcasted_iota(jnp.int32, (half, half), 1)
    key_scale = score_scale * LOG2_E
    q_lat = lat_ref[:, 0, :, :q_rank].reshape(seq, q_rank)
    kv_lat = lat_ref[:, 0, :, q_rank:q_rank + kv_rank].reshape(seq, kv_rank)
    k_rope = lat_ref[:, 0, :, q_rank + kv_rank:].reshape(seq, 128)
    half_q = wq_ref.shape[0] // 2

    def q_step(i, carry):
        at = pl.ds(pl.multiple_of(i * half_q, half_q), half_q)
        q_ref[0, at, :] = dot(wq_ref[at, :], q_lat, 1, 1).astype(BF16)
        return carry

    lax.fori_loop(0, 2, q_step, 0)
    k_buf[...] = dot(kv_lat, wk_ref[...], 1, 1).astype(BF16)
    v_buf[...] = dot(wv_ref[...], kv_lat, 1, 1).astype(BF16)
    cos, sin = cos_ref[...], sin_ref[...]

    def scores(h, side):
        at = h * head
        k_pair = k_buf[:, pl.ds((h - side) * 64, 128)]
        q_nope = q_ref[0, pl.ds(at, nope), :]
        tail = q_ref[0, pl.ds(at + nope, rope), :].astype(F32)
        lead, last = tail[:mid], tail[mid:]
        rotary = jnp.concatenate([lead * cos - last * sin, last * cos + lead * sin], axis=0).astype(BF16)
        q_ref[0, pl.ds(at + nope, rope), :] = rotary
        k = jnp.where(low, k_pair, k_rope) if side == 0 else jnp.where(low, k_rope, k_pair)
        return dot(k, fill_slot(q_nope, rotary, side), 1, 0)

    def attend(h, s):
        early = jnp.where(seen, s[:half, :half], MASKED)
        cross = s[:half, half:]
        late = jnp.where(seen, s[half:, half:], MASKED)
        peak0 = jnp.max(early, axis=0, keepdims=True)
        peak1 = jnp.maximum(jnp.max(cross, axis=0, keepdims=True), jnp.max(late, axis=0, keepdims=True))
        early = jnp.exp2((early - peak0) * key_scale)
        cross = jnp.exp2((cross - peak1) * key_scale)
        late = jnp.exp2((late - peak1) * key_scale)
        total0 = jnp.sum(early, axis=0, keepdims=True)
        total1 = jnp.sum(cross, axis=0, keepdims=True) + jnp.sum(late, axis=0, keepdims=True)
        inv0, inv1 = 1.0 / total0, 1.0 / total1
        prob = whole((early * inv0).astype(BF16), (cross * inv1).astype(BF16), (late * inv1).astype(BF16), half)
        peak = jnp.concatenate([peak0, peak1], axis=1)
        total = jnp.concatenate([total0, total1], axis=1)
        lse_ref[0, pl.ds(h, 1), :] = peak * key_scale + jnp.log2(total)
        return dot(v_buf[pl.ds(h * value, value), :], prob, 1, 0)

    def emit(pair, outs):
        o_pair = jnp.transpose(jnp.concatenate(outs, axis=0)).astype(BF16)
        o_ref[:, 0, :, pl.ds(pair * 128, 128)] = o_pair.reshape(shards, rows, 128)

    def group_step(i, carry):
        first = i * unroll * 2
        count = unroll * 2
        tiles = [scores(first + j, j % 2) if j < FORWARD_AHEAD else None for j in range(count)]
        outs = [None] * count
        for j in range(count):
            if j + FORWARD_AHEAD < count:
                tiles[j + FORWARD_AHEAD] = scores(first + j + FORWARD_AHEAD, (j + FORWARD_AHEAD) % 2)
            outs[j] = attend(first + j, tiles[j])
            if j % 2 == 1:
                emit(i * unroll + j // 2, outs[j - 1:j + 1])
        return carry

    if unroll == pairs:
        group_step(0, 0)
    else:
        lax.fori_loop(0, pairs // unroll, group_step, 0)
    o_all = o_ref[:, 0].reshape(seq, pairs * 2 * value)
    step = 512

    def out_step(i, carry):
        cols = pl.ds(pl.multiple_of(i * step, step), step)
        part_ref[:, 0, :, cols] = dot(o_all, wo_ref[:, cols], 1, 0).astype(BF16).reshape(shards, rows, step)
        return carry

    lax.fori_loop(0, part_ref.shape[3] // step, out_step, 0)


def backward_kernel(dims, score_scale, unroll, lat_ref, dy_ref, q_ref, lse_ref, wq_ref, wk_ref, wv_ref, wo_ref, cos_ref, sin_ref, glat_ref, dq_ref, dk_ref, dv_ref, do_buf, rope_acc, k_buf, kt_buf, v_buf):
    q_rank, kv_rank, nope, rope, value = dims
    shards, _, rows, _ = lat_ref.shape
    seq = shards * rows
    half = seq // 2
    head = nope + rope
    mid = rope // 2
    pairs = wk_ref.shape[0] // (2 * nope)
    low = lax.broadcasted_iota(jnp.int32, (seq, 128), 1) < 64
    seen = lax.broadcasted_iota(jnp.int32, (half, half), 0) <= lax.broadcasted_iota(jnp.int32, (half, half), 1)
    key_scale = score_scale * LOG2_E
    kv_lat = lat_ref[:, 0, :, q_rank:q_rank + kv_rank].reshape(seq, kv_rank)
    k_rope = lat_ref[:, 0, :, q_rank + kv_rank:].reshape(seq, 128)
    k_rope_t = jnp.transpose(k_rope.astype(F32))[:rope].astype(BF16)
    dy = dy_ref[:, 0].reshape(seq, dy_ref.shape[3])
    step = 256

    def grad_out_step(i, carry):
        at = pl.ds(pl.multiple_of(i * step, step), step)
        do_buf[at, :] = dot(wo_ref[at, :], dy, 1, 1).astype(BF16)
        return carry

    lax.fori_loop(0, do_buf.shape[0] // step, grad_out_step, 0)
    k_buf[...] = dot(kv_lat, wk_ref[...], 1, 1).astype(BF16)
    kt_buf[...] = dot(wk_ref[...], kv_lat, 1, 1).astype(BF16)
    v_buf[...] = dot(kv_lat, wv_ref[...], 1, 1).astype(BF16)
    rope_acc[...] = jnp.zeros_like(rope_acc)
    cos, sin = cos_ref[...], sin_ref[...]
    none = jnp.zeros((value, seq), BF16)

    def scores(h, side):
        lanes = pl.ds((h - side) * 64, 128)
        q = q_ref[0, pl.ds(h * head, head), :]
        k_pair = k_buf[:, lanes]
        k = jnp.where(low, k_pair, k_rope) if side == 0 else jnp.where(low, k_rope, k_pair)
        do = do_buf[pl.ds(h * value, value), :]
        do_slot = jnp.concatenate([do, none] if side == 0 else [none, do], axis=0)
        s = dot(k, fill_slot(q[:nope], q[nope:], side), 1, 0)
        return s, dot(v_buf[:, lanes], do_slot, 1, 0)

    def finish(h, tiles):
        s, dp = tiles
        lse = lse_ref[0, pl.ds(h, 1), :]
        p_early = jnp.exp2(jnp.where(seen, s[:half, :half], MASKED) * key_scale - lse[:, :half])
        p_cross = jnp.exp2(s[:half, half:] * key_scale - lse[:, half:])
        p_late = jnp.exp2(jnp.where(seen, s[half:, half:], MASKED) * key_scale - lse[:, half:])
        prob = whole(p_early.astype(BF16), p_cross.astype(BF16), p_late.astype(BF16), half)
        dp_early, dp_cross, dp_late = dp[:half, :half], dp[:half, half:], dp[half:, half:]
        sum0 = jnp.sum(p_early * dp_early, axis=0, keepdims=True)
        sum1 = jnp.sum(p_cross * dp_cross, axis=0, keepdims=True) + jnp.sum(p_late * dp_late, axis=0, keepdims=True)
        ds_early = (p_early * (dp_early - sum0) * score_scale).astype(BF16)
        ds_cross = (p_cross * (dp_cross - sum1) * score_scale).astype(BF16)
        ds_late = (p_late * (dp_late - sum1) * score_scale).astype(BF16)
        return prob, whole(ds_early, ds_cross, ds_late, half)

    def products(h, prob, ds):
        rows64 = pl.ds(h * 64, 64)
        grad_v = dot(do_buf[rows64, :], prob, 1, 1)
        dv_ref[0, rows64, :] = grad_v.astype(BF16)
        grad_k = dot(q_ref[0, pl.ds(h * head, head), :], ds, 1, 1)
        k_t = jnp.concatenate([kt_buf[rows64, :], k_rope_t], axis=0)
        grad_q = dot(k_t, ds, 1, 0)
        lead, last = grad_q[nope:nope + mid], grad_q[nope + mid:]
        dq_ref[0, pl.ds(h * head, head), :] = jnp.concatenate([grad_q[:nope], lead * cos + last * sin, last * cos - lead * sin], axis=0).astype(BF16)
        dk_ref[0, rows64, :] = grad_k[:nope].astype(BF16)
        rope_acc[...] += grad_k[nope:]

    def group_step(i, carry):
        count = unroll * 2
        first = i * count
        tiles = [scores(first + j, j % 2) if j < BACKWARD_AHEAD else None for j in range(count)]
        held = None
        for j in range(count):
            if j + BACKWARD_AHEAD < count:
                tiles[j + BACKWARD_AHEAD] = scores(first + j + BACKWARD_AHEAD, (j + BACKWARD_AHEAD) % 2)
            done = finish(first + j, tiles[j])
            if held is not None:
                products(first + j - 1, *held)
            held = done
        products(first + count - 1, *held)
        return carry

    if unroll == pairs:
        group_step(0, 0)
    else:
        lax.fori_loop(0, pairs // unroll, group_step, 0)
    dq, dk, dv = dq_ref[0], dk_ref[0], dv_ref[0]
    glat_ref[:, 0, :, :q_rank] = dot(dq, wq_ref[...], 0, 0).astype(BF16).reshape(shards, rows, q_rank)
    grad_kv = dot(dk, wk_ref[...], 0, 0) + dot(dv, wv_ref[...], 0, 0)
    glat_ref[:, 0, :, q_rank:q_rank + kv_rank] = grad_kv.astype(BF16).reshape(shards, rows, kv_rank)
    padded = jnp.concatenate([rope_acc[...], jnp.zeros((128 - rope, seq), F32)], axis=0)
    glat_ref[:, 0, :, q_rank + kv_rank:] = jnp.transpose(padded).astype(BF16).reshape(shards, rows, 128)


def weights_kernel(q_rank, kv_rank, lat_ref, dq_ref, dk_ref, dv_ref, gwq_ref, gwk_ref, gwv_ref):
    shards, _, rows, _ = lat_ref.shape
    seq = shards * rows
    q_lat = lat_ref[:, 0, :, :q_rank].reshape(seq, q_rank)
    kv_lat = lat_ref[:, 0, :, q_rank:q_rank + kv_rank].reshape(seq, kv_rank)
    step = 256

    @pl.when(pl.program_id(0) == 0)
    def _():
        gwq_ref[...] = jnp.zeros_like(gwq_ref)
        gwk_ref[...] = jnp.zeros_like(gwk_ref)
        gwv_ref[...] = jnp.zeros_like(gwv_ref)

    def q_step(i, carry):
        at = pl.ds(pl.multiple_of(i * step, step), step)
        gwq_ref[at, :] += dot(dq_ref[0, at, :], q_lat, 1, 0)
        return carry

    lax.fori_loop(0, gwq_ref.shape[0] // step, q_step, 0)
    gwk_ref[...] += dot(dk_ref[0], kv_lat, 1, 0)
    gwv_ref[...] += dot(dv_ref[0], kv_lat, 1, 0)


def latent_kernel(axis, x_ref, gain_ref, wdq_ref, wdkv_ref, qgain_ref, kvgain_ref, tab_ref, normed_ref, qlat_ref, kvlat_ref, lat_ref, wr_buf):
    batch, rows, dim = x_ref.shape
    count = batch * rows
    q_rank, kv_rank = qgain_ref.shape[1], kvgain_ref.shape[1]
    rope = wdkv_ref.shape[0] - kv_rank

    @pl.when(pl.program_id(0) == 0)
    def _():
        wr_buf[...] = jnp.zeros_like(wr_buf)
        wr_buf[:rope, :] = wdkv_ref[kv_rank:, :]

    def unit(v):
        return v * lax.rsqrt(jnp.mean(v * v, axis=-1, keepdims=True) + NORM_EPS)

    x = x_ref[...].reshape(count, dim).astype(F32)
    normed = (unit(x) * gain_ref[...].astype(F32)).astype(BF16)
    normed_ref[...] = normed
    q_lat = dot(normed, wdq_ref[...], 1, 0).astype(BF16)
    kv_lat = dot(normed, wdkv_ref[:kv_rank, :], 1, 1).astype(BF16)
    k_in = dot(normed, wr_buf[...], 1, 1).astype(BF16).astype(F32)
    qlat_ref[...] = q_lat
    kvlat_ref[...] = kv_lat
    lat_ref[:, :, :q_rank] = (unit(q_lat.astype(F32)) * qgain_ref[...].astype(F32)).astype(BF16).reshape(batch, rows, q_rank)
    lat_ref[:, :, q_rank:q_rank + kv_rank] = (unit(kv_lat.astype(F32)) * kvgain_ref[...].astype(F32)).astype(BF16).reshape(batch, rows, kv_rank)
    here = pl.ds(pl.multiple_of(lax.axis_index(axis) * rows, rows), rows)
    tab = jnp.concatenate([tab_ref[here, :]] * batch, axis=0)
    mid = rope // 2
    k_rot = k_in * tab[:, :128] + pltpu.roll(k_in, 128 - mid, 1) * tab[:, 128:256] + pltpu.roll(k_in, mid, 1) * tab[:, 256:]
    lat_ref[:, :, q_rank + kv_rank:] = (k_rot + pltpu.roll(k_rot, 64, 1)).astype(BF16).reshape(batch, rows, 128)


def solution(mesh):
    act_spec = P('dp', 'tp', None)
    head_spec = P(None, 'tp', None)
    in_specs = (act_spec, P(None), P(None, None), P(None), P(None, None), P(None), head_spec, head_spec, head_spec, head_spec, P('tp', None, None), P(None, None), P(None, None), act_spec)
    grad_head_spec = P('dp', 'tp', None)
    out_specs = (act_spec, act_spec, P('dp'), P('dp', None), P('dp'), P('dp', None), P('dp'), grad_head_spec, grad_head_spec, grad_head_spec, grad_head_spec, P(('dp', 'tp'), None, None))

    def local_step(hidden, norm_gain, w_dq, q_gain, w_dkv, kv_gain, w_uq, w_qr, w_uk, w_uv, w_out, rope_cos, rope_sin, grad_out):
        shards = mesh.shape['tp']
        batch, rows, dim = hidden.shape
        q_rank, kv_rank = q_gain.shape[0], kv_gain.shape[0]
        heads, nope = w_uq.shape[1:]
        rope = w_qr.shape[2]
        mid = rope // 2
        value = w_uv.shape[2]
        seq = shards * rows
        tokens = batch * seq
        here = batch * rows
        lat_width = q_rank + kv_rank + 128
        kv_width = kv_rank + rope
        score_scale = (nope + rope) ** -0.5

        x2 = hidden.reshape(here, dim)
        none = jnp.zeros((seq, 128 - rope), F32)
        half_none = jnp.zeros((seq, mid), F32)
        key_tab = jnp.concatenate([rope_cos, rope_cos, none, -rope_sin, half_none, none, half_none, rope_sin, none], axis=1)
        some = min(batch, 4)
        normed, q_latent, kv_latent, lat_here = pl.pallas_call(
            functools.partial(latent_kernel, 'tp'),
            grid=(batch // some,),
            in_specs=[pl.BlockSpec((some, rows, dim), lambda b: (b, 0, 0))] + [pl.BlockSpec(shape, lambda b: (0, 0)) for shape in ((1, dim), w_dq.shape, (kv_width, dim), (1, q_rank), (1, kv_rank), key_tab.shape)],
            out_specs=[pl.BlockSpec((some * rows, width), lambda b: (b, 0)) for width in (dim, q_rank, kv_rank)] + [pl.BlockSpec((some, rows, lat_width), lambda b: (b, 0, 0))],
            out_shape=[jax.ShapeDtypeStruct((here, width), BF16) for width in (dim, q_rank, kv_rank)] + [jax.ShapeDtypeStruct((batch, rows, lat_width), BF16)],
            scratch_shapes=[pltpu.VMEM((128, dim), BF16)],
            compiler_params=pltpu.CompilerParams(dimension_semantics=("arbitrary",)),
            cost_estimate=pl.CostEstimate(flops=2 * here * dim * (q_rank + kv_width), bytes_accessed=12_000_000, transcendentals=here),
            name="latents",
        )(hidden, norm_gain[None], w_dq, w_dkv.T, q_gain[None], kv_gain[None], key_tab)
        lat_all = lax.all_gather(lat_here, 'tp', axis=0)
        dy_all = lax.all_gather(grad_out, 'tp', axis=0)

        wq = jnp.concatenate([w_uq.transpose(1, 2, 0), w_qr.transpose(1, 2, 0)], axis=1).reshape(heads * (nope + rope), q_rank)
        wk = w_uk.transpose(1, 2, 0).reshape(heads * nope, kv_rank)
        wv = w_uv.transpose(1, 2, 0).reshape(heads * value, kv_rank)
        w_o = w_out.reshape(heads * value, dim)
        weights = (wq, wk, wv, w_o, rope_cos.T, rope_sin.T)
        dims = (q_rank, kv_rank, nope, rope, value)

        def tok(width):
            return pl.BlockSpec((shards, 1, rows, width), lambda b: (0, b, 0, 0))

        def fixed(shape):
            return pl.BlockSpec(shape, lambda b: (0,) * len(shape))

        def per_batch(shape):
            return pl.BlockSpec((1,) + shape, lambda b: (b,) + (0,) * len(shape))

        def out(width):
            return jax.ShapeDtypeStruct((shards, batch, rows, width), BF16)

        weight_specs = [fixed(w.shape) for w in weights]
        attn_flops = 2 * batch * heads * seq * seq * 256
        up_flops = 2 * tokens * heads * ((nope + rope) * q_rank + (nope + value) * kv_rank)
        out_flops = 2 * tokens * heads * value * dim
        q_all, o_all, lse_all, attn_part = pl.pallas_call(
            functools.partial(forward_kernel, dims, score_scale, heads // 2),
            grid=(batch,),
            in_specs=[tok(lat_width)] + weight_specs,
            out_specs=[per_batch((wq.shape[0], seq)), tok(heads * value), per_batch((heads, seq)), tok(dim)],
            out_shape=[jax.ShapeDtypeStruct((batch, wq.shape[0], seq), BF16), out(heads * value), jax.ShapeDtypeStruct((batch, heads, seq), F32), out(dim)],
            scratch_shapes=[pltpu.VMEM((seq, heads * nope), BF16), pltpu.VMEM((heads * value, seq), BF16)],
            compiler_params=pltpu.CompilerParams(dimension_semantics=("arbitrary",)),
            cost_estimate=pl.CostEstimate(flops=attn_flops + up_flops + out_flops, bytes_accessed=70_000_000, transcendentals=batch * heads * seq * seq),
            name="attn_forward",
        )(lat_all, *weights)
        attn_out = lax.psum_scatter(attn_part, 'tp', scatter_dimension=0, tiled=False)
        out_hidden = (hidden.astype(F32) + attn_out.astype(F32)).astype(BF16)

        glat, dq_all, dk_all, dv_all = pl.pallas_call(
            functools.partial(backward_kernel, dims, score_scale, heads // 2),
            grid=(batch,),
            in_specs=[tok(lat_width), tok(dim), per_batch((wq.shape[0], seq)), per_batch((heads, seq))] + weight_specs,
            out_specs=[tok(lat_width)] + [per_batch((w.shape[0], seq)) for w in (wq, wk, wv)],
            out_shape=[out(lat_width)] + [jax.ShapeDtypeStruct((batch, w.shape[0], seq), BF16) for w in (wq, wk, wv)],
            scratch_shapes=[pltpu.VMEM((heads * value, seq), BF16), pltpu.VMEM((rope, seq), F32), pltpu.VMEM((seq, heads * nope), BF16), pltpu.VMEM((heads * nope, seq), BF16), pltpu.VMEM((seq, heads * value), BF16)],
            compiler_params=pltpu.CompilerParams(dimension_semantics=("arbitrary",)),
            cost_estimate=pl.CostEstimate(flops=3 * attn_flops + 2 * up_flops + out_flops, bytes_accessed=60_000_000, transcendentals=batch * heads * seq * seq),
            name="attn_backward",
        )(lat_all, dy_all, q_all, lse_all, *weights)
        grad_lat = lax.psum_scatter(glat, 'tp', scatter_dimension=0, tiled=False)
        grad_lat = grad_lat.reshape(here, lat_width).astype(F32)

        gwq, gwk, gwv = pl.pallas_call(
            functools.partial(weights_kernel, q_rank, kv_rank),
            grid=(batch,),
            in_specs=[tok(lat_width)] + [per_batch((w.shape[0], seq)) for w in (wq, wk, wv)],
            out_specs=[fixed(w.shape) for w in (wq, wk, wv)],
            out_shape=[jax.ShapeDtypeStruct(w.shape, F32) for w in (wq, wk, wv)],
            compiler_params=pltpu.CompilerParams(dimension_semantics=("arbitrary",)),
            cost_estimate=pl.CostEstimate(flops=up_flops, bytes_accessed=50_000_000, transcendentals=0),
            name="head_weight_grads",
        )(lat_all, dq_all, dk_all, dv_all)
        grad_wq = gwq.reshape(heads, nope + rope, q_rank)
        grad_w_uq = grad_wq[:, :nope].transpose(2, 0, 1)
        grad_w_qr = grad_wq[:, nope:].transpose(2, 0, 1)
        grad_w_uk = gwk.reshape(heads, nope, kv_rank).transpose(2, 0, 1)
        grad_w_uv = gwv.reshape(heads, value, kv_rank).transpose(2, 0, 1)
        grad_w_out = dot(o_all.reshape(tokens, heads * value), dy_all.reshape(tokens, dim), 0, 0).reshape(heads, value, dim)

        _, x_unit, x_inv = norm_forward(x2, norm_gain)
        _, q_unit, q_inv = norm_forward(q_latent, q_gain)
        _, kv_unit, kv_inv = norm_forward(kv_latent, kv_gain)
        place = lax.axis_index('tp') * rows
        cos_here = jnp.tile(lax.dynamic_slice_in_dim(rope_cos, place, rows, 0), (batch, 1))
        sin_here = jnp.tile(lax.dynamic_slice_in_dim(rope_sin, place, rows, 0), (batch, 1))
        grad_q_lat, grad_q_gain = norm_backward(grad_lat[:, :q_rank], q_unit, q_inv, q_gain)
        grad_kv_lat, grad_kv_gain = norm_backward(grad_lat[:, q_rank:q_rank + kv_rank], kv_unit, kv_inv, kv_gain)
        gk = grad_lat[:, q_rank + kv_rank:q_rank + kv_rank + rope]
        gk_lead, gk_tail = gk[:, :mid], gk[:, mid:]
        grad_q_lat = grad_q_lat.astype(BF16)
        grad_kv_all = jnp.concatenate([grad_kv_lat, gk_lead * cos_here + gk_tail * sin_here, gk_tail * cos_here - gk_lead * sin_here], axis=1).astype(BF16)
        own = dim // shards
        own_kv = kv_width // shards * dim // q_rank
        part_dq = dot(normed, grad_q_lat, 0, 0).astype(BF16).reshape(shards, own, q_rank)
        part_dkv = dot(grad_kv_all, normed, 0, 0).astype(BF16).reshape(shards, own_kv, q_rank)
        down_sum = lax.psum_scatter(jnp.concatenate([part_dq, part_dkv], axis=1), 'tp', scatter_dimension=0, tiled=False)
        grad_normed = dot(grad_q_lat, w_dq, 1, 1) + dot(grad_kv_all, w_dkv, 1, 1)
        grad_x_norm, grad_norm_gain = norm_backward(grad_normed, x_unit, x_inv, norm_gain)
        grad_hidden = grad_out.reshape(here, dim).astype(F32) + grad_x_norm

        gains = jnp.concatenate([grad_norm_gain, grad_q_gain, grad_kv_gain])
        gain_rows = -(-gains.shape[0] // q_rank)
        gains = jnp.pad(gains, (0, gain_rows * q_rank - gains.shape[0])).reshape(gain_rows, q_rank)
        high = lax.reduce_precision(gains, 8, 7)
        middle = lax.reduce_precision(gains - high, 8, 7)
        tail = gains - high - middle
        packed = jnp.concatenate([down_sum, high.astype(BF16), middle.astype(BF16), tail.astype(BF16)], axis=0)
        gathered = lax.all_gather(packed, 'tp', axis=0)
        grad_w_dq = gathered[:, :own].reshape(dim, q_rank).astype(F32)
        grad_w_dkv = gathered[:, own:own + own_kv].reshape(kv_width, dim).astype(F32).T
        terms = gathered[:, own + own_kv:].astype(F32).reshape(shards, 3, gain_rows * q_rank)
        sums = jnp.sum(terms[:, 0] + terms[:, 1] + terms[:, 2], axis=0)
        g_norm = sums[:dim]
        g_q = sums[dim:dim + q_rank]
        g_kv = sums[dim + q_rank:dim + q_rank + kv_rank]
        return (out_hidden, grad_hidden.reshape(batch, rows, dim), g_norm, grad_w_dq, g_q, grad_w_dkv, g_kv, grad_w_uq, grad_w_qr, grad_w_uk, grad_w_uv, grad_w_out)

    return jax.shard_map(local_step, mesh=mesh, in_specs=in_specs, out_specs=out_specs, check_vma=False)
```

```python
import functools

import jax
import jax.numpy as jnp
from jax import lax
from jax.experimental import pallas as pl
from jax.experimental.pallas import tpu as pltpu
from jax.sharding import PartitionSpec as P


NORM_EPS = 1e-6
LOG2_E = 1.4426950408889634
MASKED = -1e30
FORWARD_AHEAD = 4
BACKWARD_AHEAD = 2
F32 = jnp.float32
BF16 = jnp.bfloat16


def norm_forward(value, gain_vec):
    value32 = value.astype(F32)
    inv_rms = lax.rsqrt(jnp.mean(value32 * value32, axis=-1, keepdims=True) + NORM_EPS)
    unit_val = value32 * inv_rms
    return (unit_val * gain_vec.astype(F32)).astype(BF16), unit_val, inv_rms


def norm_backward(grad_norm, unit_val, inv_rms, gain_vec):
    grad_unit = grad_norm * gain_vec.astype(F32)
    grad_in = inv_rms * (grad_unit - unit_val * jnp.mean(grad_unit * unit_val, axis=-1, keepdims=True))
    grad_gain = jnp.sum(grad_norm * unit_val, axis=tuple(range(grad_norm.ndim - 1)))
    return grad_in, grad_gain


def dot(lhs, rhs, lhs_dim, rhs_dim):
    return lax.dot_general(lhs, rhs, (((lhs_dim,), (rhs_dim,)), ((), ())), preferred_element_type=F32)


def whole(early, cross, late, half):
    blank = jnp.zeros((half, half), BF16)
    return jnp.concatenate([jnp.concatenate([early, cross], axis=1), jnp.concatenate([blank, late], axis=1)], axis=0)


def fill_slot(nope, rotary, side):
    blank = jnp.zeros((128 - nope.shape[0] - rotary.shape[0], nope.shape[1]), nope.dtype)
    parts = [nope, rotary, blank] if side == 0 else [rotary, blank, nope]
    return jnp.concatenate(parts, axis=0)


def forward_kernel(dims, score_scale, unroll, lat_ref, wq_ref, wk_ref, wv_ref, wo_ref, cos_ref, sin_ref, q_ref, o_ref, lse_ref, part_ref, k_buf, v_buf):
    q_rank, kv_rank, nope, rope, value = dims
    shards, _, rows, _ = lat_ref.shape
    seq = shards * rows
    half = seq // 2
    head = nope + rope
    mid = rope // 2
    pairs = wk_ref.shape[0] // (2 * nope)
    low = lax.broadcasted_iota(jnp.int32, (seq, 128), 1) < 64
    seen = lax.broadcasted_iota(jnp.int32, (half, half), 0) <= lax.broadcasted_iota(jnp.int32, (half, half), 1)
    key_scale = score_scale * LOG2_E
    q_lat = lat_ref[:, 0, :, :q_rank].reshape(seq, q_rank)
    kv_lat = lat_ref[:, 0, :, q_rank:q_rank + kv_rank].reshape(seq, kv_rank)
    k_rope = lat_ref[:, 0, :, q_rank + kv_rank:].reshape(seq, 128)
    half_q = wq_ref.shape[0] // 2

    def q_step(i, carry):
        at = pl.ds(pl.multiple_of(i * half_q, half_q), half_q)
        q_ref[0, at, :] = dot(wq_ref[at, :], q_lat, 1, 1).astype(BF16)
        return carry

    lax.fori_loop(0, 2, q_step, 0)
    k_buf[...] = dot(kv_lat, wk_ref[...], 1, 1).astype(BF16)
    v_buf[...] = dot(wv_ref[...], kv_lat, 1, 1).astype(BF16)
    cos, sin = cos_ref[...], sin_ref[...]

    def scores(h, side):
        at = h * head
        k_pair = k_buf[:, pl.ds((h - side) * 64, 128)]
        q_nope = q_ref[0, pl.ds(at, nope), :]
        tail = q_ref[0, pl.ds(at + nope, rope), :].astype(F32)
        lead, last = tail[:mid], tail[mid:]
        rotary = jnp.concatenate([lead * cos - last * sin, last * cos + lead * sin], axis=0).astype(BF16)
        q_ref[0, pl.ds(at + nope, rope), :] = rotary
        k = jnp.where(low, k_pair, k_rope) if side == 0 else jnp.where(low, k_rope, k_pair)
        return dot(k, fill_slot(q_nope, rotary, side), 1, 0)

    def attend(h, s):
        early = jnp.where(seen, s[:half, :half], MASKED)
        cross = s[:half, half:]
        late = jnp.where(seen, s[half:, half:], MASKED)
        peak0 = jnp.max(early, axis=0, keepdims=True)
        peak1 = jnp.maximum(jnp.max(cross, axis=0, keepdims=True), jnp.max(late, axis=0, keepdims=True))
        early = jnp.exp2((early - peak0) * key_scale)
        cross = jnp.exp2((cross - peak1) * key_scale)
        late = jnp.exp2((late - peak1) * key_scale)
        total0 = jnp.sum(early, axis=0, keepdims=True)
        total1 = jnp.sum(cross, axis=0, keepdims=True) + jnp.sum(late, axis=0, keepdims=True)
        inv0, inv1 = 1.0 / total0, 1.0 / total1
        prob = whole((early * inv0).astype(BF16), (cross * inv1).astype(BF16), (late * inv1).astype(BF16), half)
        peak = jnp.concatenate([peak0, peak1], axis=1)
        total = jnp.concatenate([total0, total1], axis=1)
        lse_ref[0, pl.ds(h, 1), :] = peak * key_scale + jnp.log2(total)
        return dot(v_buf[pl.ds(h * value, value), :], prob, 1, 0)

    def emit(pair, outs):
        o_pair = jnp.transpose(jnp.concatenate(outs, axis=0)).astype(BF16)
        o_ref[:, 0, :, pl.ds(pair * 128, 128)] = o_pair.reshape(shards, rows, 128)

    def group_step(i, carry):
        first = i * unroll * 2
        count = unroll * 2
        tiles = [scores(first + j, j % 2) if j < FORWARD_AHEAD else None for j in range(count)]
        outs = [None] * count
        for j in range(count):
            if j + FORWARD_AHEAD < count:
                tiles[j + FORWARD_AHEAD] = scores(first + j + FORWARD_AHEAD, (j + FORWARD_AHEAD) % 2)
            outs[j] = attend(first + j, tiles[j])
            if j % 2 == 1:
                emit(i * unroll + j // 2, outs[j - 1:j + 1])
        return carry

    if unroll == pairs:
        group_step(0, 0)
    else:
        lax.fori_loop(0, pairs // unroll, group_step, 0)
    o_all = o_ref[:, 0].reshape(seq, pairs * 2 * value)
    step = 512

    def out_step(i, carry):
        cols = pl.ds(pl.multiple_of(i * step, step), step)
        part_ref[:, 0, :, cols] = dot(o_all, wo_ref[:, cols], 1, 0).astype(BF16).reshape(shards, rows, step)
        return carry

    lax.fori_loop(0, part_ref.shape[3] // step, out_step, 0)


def backward_kernel(dims, score_scale, unroll, lat_ref, dy_ref, q_ref, lse_ref, wq_ref, wk_ref, wv_ref, wo_ref, cos_ref, sin_ref, glat_ref, dq_ref, dk_ref, dv_ref, do_buf, rope_acc, k_buf, kt_buf, v_buf):
    q_rank, kv_rank, nope, rope, value = dims
    shards, _, rows, _ = lat_ref.shape
    seq = shards * rows
    half = seq // 2
    head = nope + rope
    mid = rope // 2
    pairs = wk_ref.shape[0] // (2 * nope)
    low = lax.broadcasted_iota(jnp.int32, (seq, 128), 1) < 64
    seen = lax.broadcasted_iota(jnp.int32, (half, half), 0) <= lax.broadcasted_iota(jnp.int32, (half, half), 1)
    key_scale = score_scale * LOG2_E
    kv_lat = lat_ref[:, 0, :, q_rank:q_rank + kv_rank].reshape(seq, kv_rank)
    k_rope = lat_ref[:, 0, :, q_rank + kv_rank:].reshape(seq, 128)
    k_rope_t = jnp.transpose(k_rope.astype(F32))[:rope].astype(BF16)
    dy = dy_ref[:, 0].reshape(seq, dy_ref.shape[3])
    step = 256

    def grad_out_step(i, carry):
        at = pl.ds(pl.multiple_of(i * step, step), step)
        do_buf[at, :] = dot(wo_ref[at, :], dy, 1, 1).astype(BF16)
        return carry

    lax.fori_loop(0, do_buf.shape[0] // step, grad_out_step, 0)
    k_buf[...] = dot(kv_lat, wk_ref[...], 1, 1).astype(BF16)
    kt_buf[...] = dot(wk_ref[...], kv_lat, 1, 1).astype(BF16)
    v_buf[...] = dot(kv_lat, wv_ref[...], 1, 1).astype(BF16)
    rope_acc[...] = jnp.zeros_like(rope_acc)
    cos, sin = cos_ref[...], sin_ref[...]
    none = jnp.zeros((value, seq), BF16)

    def scores(h, side):
        lanes = pl.ds((h - side) * 64, 128)
        q = q_ref[0, pl.ds(h * head, head), :]
        k_pair = k_buf[:, lanes]
        k = jnp.where(low, k_pair, k_rope) if side == 0 else jnp.where(low, k_rope, k_pair)
        do = do_buf[pl.ds(h * value, value), :]
        do_slot = jnp.concatenate([do, none] if side == 0 else [none, do], axis=0)
        s = dot(k, fill_slot(q[:nope], q[nope:], side), 1, 0)
        return s, dot(v_buf[:, lanes], do_slot, 1, 0)

    def finish(h, tiles):
        s, dp = tiles
        lse = lse_ref[0, pl.ds(h, 1), :]
        p_early = jnp.exp2(jnp.where(seen, s[:half, :half], MASKED) * key_scale - lse[:, :half])
        p_cross = jnp.exp2(s[:half, half:] * key_scale - lse[:, half:])
        p_late = jnp.exp2(jnp.where(seen, s[half:, half:], MASKED) * key_scale - lse[:, half:])
        prob = whole(p_early.astype(BF16), p_cross.astype(BF16), p_late.astype(BF16), half)
        dp_early, dp_cross, dp_late = dp[:half, :half], dp[:half, half:], dp[half:, half:]
        sum0 = jnp.sum(p_early * dp_early, axis=0, keepdims=True)
        sum1 = jnp.sum(p_cross * dp_cross, axis=0, keepdims=True) + jnp.sum(p_late * dp_late, axis=0, keepdims=True)
        ds_early = (p_early * (dp_early - sum0) * score_scale).astype(BF16)
        ds_cross = (p_cross * (dp_cross - sum1) * score_scale).astype(BF16)
        ds_late = (p_late * (dp_late - sum1) * score_scale).astype(BF16)
        return prob, whole(ds_early, ds_cross, ds_late, half)

    def products(h, prob, ds):
        rows64 = pl.ds(h * 64, 64)
        grad_v = dot(do_buf[rows64, :], prob, 1, 1)
        dv_ref[0, rows64, :] = grad_v.astype(BF16)
        grad_k = dot(q_ref[0, pl.ds(h * head, head), :], ds, 1, 1)
        k_t = jnp.concatenate([kt_buf[rows64, :], k_rope_t], axis=0)
        grad_q = dot(k_t, ds, 1, 0)
        lead, last = grad_q[nope:nope + mid], grad_q[nope + mid:]
        dq_ref[0, pl.ds(h * head, head), :] = jnp.concatenate([grad_q[:nope], lead * cos + last * sin, last * cos - lead * sin], axis=0).astype(BF16)
        dk_ref[0, rows64, :] = grad_k[:nope].astype(BF16)
        rope_acc[...] += grad_k[nope:]

    def group_step(i, carry):
        count = unroll * 2
        first = i * count
        tiles = [scores(first + j, j % 2) if j < BACKWARD_AHEAD else None for j in range(count)]
        held = None
        for j in range(count):
            if j + BACKWARD_AHEAD < count:
                tiles[j + BACKWARD_AHEAD] = scores(first + j + BACKWARD_AHEAD, (j + BACKWARD_AHEAD) % 2)
            done = finish(first + j, tiles[j])
            if held is not None:
                products(first + j - 1, *held)
            held = done
        products(first + count - 1, *held)
        return carry

    if unroll == pairs:
        group_step(0, 0)
    else:
        lax.fori_loop(0, pairs // unroll, group_step, 0)
    dq, dk, dv = dq_ref[0], dk_ref[0], dv_ref[0]
    glat_ref[:, 0, :, :q_rank] = dot(dq, wq_ref[...], 0, 0).astype(BF16).reshape(shards, rows, q_rank)
    grad_kv = dot(dk, wk_ref[...], 0, 0) + dot(dv, wv_ref[...], 0, 0)
    glat_ref[:, 0, :, q_rank:q_rank + kv_rank] = grad_kv.astype(BF16).reshape(shards, rows, kv_rank)
    padded = jnp.concatenate([rope_acc[...], jnp.zeros((128 - rope, seq), F32)], axis=0)
    glat_ref[:, 0, :, q_rank + kv_rank:] = jnp.transpose(padded).astype(BF16).reshape(shards, rows, 128)


def weights_kernel(first, width, lat_ref, *refs):
    shards, batch, rows, _ = lat_ref.shape
    seq = shards * rows
    count = len(refs) // 2

    @pl.when(pl.program_id(0) == 0)
    def _():
        for out_ref in refs[count:]:
            out_ref[...] = jnp.zeros_like(out_ref)

    step = 512
    lats = [lat_ref[:, j, :, first:first + width].reshape(seq, width) for j in range(batch)]
    for grad_ref, out_ref in zip(refs[:count], refs[count:]):
        for i in range(0, out_ref.shape[0], step):
            at = pl.ds(i, step)
            out_ref[at, :] += sum(dot(grad_ref[j, at, :], lats[j], 1, 0) for j in range(batch))


def latent_kernel(axis, x_ref, gain_ref, wdq_ref, wdkv_ref, qgain_ref, kvgain_ref, tab_ref, normed_ref, qlat_ref, kvlat_ref, lat_ref, wr_buf):
    batch, rows, dim = x_ref.shape
    count = batch * rows
    q_rank, kv_rank = qgain_ref.shape[1], kvgain_ref.shape[1]
    rope = wdkv_ref.shape[0] - kv_rank

    @pl.when(pl.program_id(0) == 0)
    def _():
        wr_buf[...] = jnp.zeros_like(wr_buf)
        wr_buf[:rope, :] = wdkv_ref[kv_rank:, :]

    def unit(v):
        return v * lax.rsqrt(jnp.mean(v * v, axis=-1, keepdims=True) + NORM_EPS)

    x = x_ref[...].reshape(count, dim).astype(F32)
    normed = (unit(x) * gain_ref[...].astype(F32)).astype(BF16)
    normed_ref[...] = normed
    q_lat = dot(normed, wdq_ref[...], 1, 0).astype(BF16)
    kv_lat = dot(normed, wdkv_ref[:kv_rank, :], 1, 1).astype(BF16)
    k_in = dot(normed, wr_buf[...], 1, 1).astype(BF16).astype(F32)
    qlat_ref[...] = q_lat
    kvlat_ref[...] = kv_lat
    lat_ref[:, :, :q_rank] = (unit(q_lat.astype(F32)) * qgain_ref[...].astype(F32)).astype(BF16).reshape(batch, rows, q_rank)
    lat_ref[:, :, q_rank:q_rank + kv_rank] = (unit(kv_lat.astype(F32)) * kvgain_ref[...].astype(F32)).astype(BF16).reshape(batch, rows, kv_rank)
    here = pl.ds(pl.multiple_of(lax.axis_index(axis) * rows, rows), rows)
    tab = jnp.concatenate([tab_ref[here, :]] * batch, axis=0)
    mid = rope // 2
    k_rot = k_in * tab[:, :128] + pltpu.roll(k_in, 128 - mid, 1) * tab[:, 128:256] + pltpu.roll(k_in, mid, 1) * tab[:, 256:]
    lat_ref[:, :, q_rank + kv_rank:] = (k_rot + pltpu.roll(k_rot, 64, 1)).astype(BF16).reshape(batch, rows, 128)


def solution(mesh):
    act_spec = P('dp', 'tp', None)
    head_spec = P(None, 'tp', None)
    in_specs = (act_spec, P(None), P(None, None), P(None), P(None, None), P(None), head_spec, head_spec, head_spec, head_spec, P('tp', None, None), P(None, None), P(None, None), act_spec)
    grad_head_spec = P('dp', 'tp', None)
    out_specs = (act_spec, act_spec, P('dp'), P('dp', None), P('dp'), P('dp', None), P('dp'), grad_head_spec, grad_head_spec, grad_head_spec, grad_head_spec, P(('dp', 'tp'), None, None))

    def local_step(hidden, norm_gain, w_dq, q_gain, w_dkv, kv_gain, w_uq, w_qr, w_uk, w_uv, w_out, rope_cos, rope_sin, grad_out):
        shards = mesh.shape['tp']
        batch, rows, dim = hidden.shape
        q_rank, kv_rank = q_gain.shape[0], kv_gain.shape[0]
        heads, nope = w_uq.shape[1:]
        rope = w_qr.shape[2]
        mid = rope // 2
        value = w_uv.shape[2]
        seq = shards * rows
        tokens = batch * seq
        here = batch * rows
        lat_width = q_rank + kv_rank + 128
        kv_width = kv_rank + rope
        score_scale = (nope + rope) ** -0.5

        x2 = hidden.reshape(here, dim)
        none = jnp.zeros((seq, 128 - rope), F32)
        half_none = jnp.zeros((seq, mid), F32)
        key_tab = jnp.concatenate([rope_cos, rope_cos, none, -rope_sin, half_none, none, half_none, rope_sin, none], axis=1)
        some = min(batch, 4)
        normed, q_latent, kv_latent, lat_here = pl.pallas_call(
            functools.partial(latent_kernel, 'tp'),
            grid=(batch // some,),
            in_specs=[pl.BlockSpec((some, rows, dim), lambda b: (b, 0, 0))] + [pl.BlockSpec(shape, lambda b: (0, 0)) for shape in ((1, dim), w_dq.shape, (kv_width, dim), (1, q_rank), (1, kv_rank), key_tab.shape)],
            out_specs=[pl.BlockSpec((some * rows, width), lambda b: (b, 0)) for width in (dim, q_rank, kv_rank)] + [pl.BlockSpec((some, rows, lat_width), lambda b: (b, 0, 0))],
            out_shape=[jax.ShapeDtypeStruct((here, width), BF16) for width in (dim, q_rank, kv_rank)] + [jax.ShapeDtypeStruct((batch, rows, lat_width), BF16)],
            scratch_shapes=[pltpu.VMEM((128, dim), BF16)],
            compiler_params=pltpu.CompilerParams(dimension_semantics=("arbitrary",)),
            cost_estimate=pl.CostEstimate(flops=2 * here * dim * (q_rank + kv_width), bytes_accessed=12_000_000, transcendentals=here),
            name="latents",
        )(hidden, norm_gain[None], w_dq, w_dkv.T, q_gain[None], kv_gain[None], key_tab)
        lat_all = lax.all_gather(lat_here, 'tp', axis=0)
        dy_all = lax.all_gather(grad_out, 'tp', axis=0)

        wq = jnp.concatenate([w_uq.transpose(1, 2, 0), w_qr.transpose(1, 2, 0)], axis=1).reshape(heads * (nope + rope), q_rank)
        wk = w_uk.transpose(1, 2, 0).reshape(heads * nope, kv_rank)
        wv = w_uv.transpose(1, 2, 0).reshape(heads * value, kv_rank)
        w_o = w_out.reshape(heads * value, dim)
        weights = (wq, wk, wv, w_o, rope_cos.T, rope_sin.T)
        dims = (q_rank, kv_rank, nope, rope, value)

        def tok(width):
            return pl.BlockSpec((shards, 1, rows, width), lambda b: (0, b, 0, 0))

        def fixed(shape):
            return pl.BlockSpec(shape, lambda b: (0,) * len(shape))

        def per_batch(shape):
            return pl.BlockSpec((1,) + shape, lambda b: (b,) + (0,) * len(shape))

        def out(width):
            return jax.ShapeDtypeStruct((shards, batch, rows, width), BF16)

        weight_specs = [fixed(w.shape) for w in weights]
        attn_flops = 2 * batch * heads * seq * seq * 256
        up_flops = 2 * tokens * heads * ((nope + rope) * q_rank + (nope + value) * kv_rank)
        out_flops = 2 * tokens * heads * value * dim
        q_all, o_all, lse_all, attn_part = pl.pallas_call(
            functools.partial(forward_kernel, dims, score_scale, heads // 2),
            grid=(batch,),
            in_specs=[tok(lat_width)] + weight_specs,
            out_specs=[per_batch((wq.shape[0], seq)), tok(heads * value), per_batch((heads, seq)), tok(dim)],
            out_shape=[jax.ShapeDtypeStruct((batch, wq.shape[0], seq), BF16), out(heads * value), jax.ShapeDtypeStruct((batch, heads, seq), F32), out(dim)],
            scratch_shapes=[pltpu.VMEM((seq, heads * nope), BF16), pltpu.VMEM((heads * value, seq), BF16)],
            compiler_params=pltpu.CompilerParams(dimension_semantics=("arbitrary",)),
            cost_estimate=pl.CostEstimate(flops=attn_flops + up_flops + out_flops, bytes_accessed=70_000_000, transcendentals=batch * heads * seq * seq),
            name="attn_forward",
        )(lat_all, *weights)
        attn_out = lax.psum_scatter(attn_part, 'tp', scatter_dimension=0, tiled=False)
        out_hidden = (hidden.astype(F32) + attn_out.astype(F32)).astype(BF16)

        glat, dq_all, dk_all, dv_all = pl.pallas_call(
            functools.partial(backward_kernel, dims, score_scale, heads // 2),
            grid=(batch,),
            in_specs=[tok(lat_width), tok(dim), per_batch((wq.shape[0], seq)), per_batch((heads, seq))] + weight_specs,
            out_specs=[tok(lat_width)] + [per_batch((w.shape[0], seq)) for w in (wq, wk, wv)],
            out_shape=[out(lat_width)] + [jax.ShapeDtypeStruct((batch, w.shape[0], seq), BF16) for w in (wq, wk, wv)],
            scratch_shapes=[pltpu.VMEM((heads * value, seq), BF16), pltpu.VMEM((rope, seq), F32), pltpu.VMEM((seq, heads * nope), BF16), pltpu.VMEM((heads * nope, seq), BF16), pltpu.VMEM((seq, heads * value), BF16)],
            compiler_params=pltpu.CompilerParams(dimension_semantics=("arbitrary",)),
            cost_estimate=pl.CostEstimate(flops=3 * attn_flops + 2 * up_flops + out_flops, bytes_accessed=60_000_000, transcendentals=batch * heads * seq * seq),
            name="attn_backward",
        )(lat_all, dy_all, q_all, lse_all, *weights)
        grad_lat = lax.psum_scatter(glat, 'tp', scatter_dimension=0, tiled=False)
        grad_lat = grad_lat.reshape(here, lat_width).astype(F32)

        many = 4 if batch % 4 == 0 else 1

        def weight_grads(first, width, grads):
            shapes = [(g.shape[1], width) for g in grads]
            return pl.pallas_call(
                functools.partial(weights_kernel, first, width),
                grid=(batch // many,),
                in_specs=[pl.BlockSpec((shards, many, rows, lat_width), lambda b: (0, b, 0, 0))] + [pl.BlockSpec((many,) + g.shape[1:], lambda b: (b, 0, 0)) for g in grads],
                out_specs=[fixed(shape) for shape in shapes],
                out_shape=[jax.ShapeDtypeStruct(shape, F32) for shape in shapes],
                compiler_params=pltpu.CompilerParams(dimension_semantics=("arbitrary",)),
                cost_estimate=pl.CostEstimate(flops=2 * tokens * width * sum(shape[0] for shape in shapes), bytes_accessed=30_000_000, transcendentals=0),
            )(lat_all, *grads)

        gwq, = weight_grads(0, q_rank, [dq_all])
        grad_wq = gwq.reshape(heads, nope + rope, q_rank)
        grad_w_uq = grad_wq[:, :nope].transpose(2, 0, 1)
        grad_w_qr = grad_wq[:, nope:].transpose(2, 0, 1)
        grad_w_out = dot(o_all.reshape(tokens, heads * value), dy_all.reshape(tokens, dim), 0, 0).reshape(heads, value, dim)

        _, x_unit, x_inv = norm_forward(x2, norm_gain)
        _, q_unit, q_inv = norm_forward(q_latent, q_gain)
        _, kv_unit, kv_inv = norm_forward(kv_latent, kv_gain)
        place = lax.axis_index('tp') * rows
        cos_here = jnp.tile(lax.dynamic_slice_in_dim(rope_cos, place, rows, 0), (batch, 1))
        sin_here = jnp.tile(lax.dynamic_slice_in_dim(rope_sin, place, rows, 0), (batch, 1))
        grad_q_lat, grad_q_gain = norm_backward(grad_lat[:, :q_rank], q_unit, q_inv, q_gain)
        grad_kv_lat, grad_kv_gain = norm_backward(grad_lat[:, q_rank:q_rank + kv_rank], kv_unit, kv_inv, kv_gain)
        gk = grad_lat[:, q_rank + kv_rank:q_rank + kv_rank + rope]
        gk_lead, gk_tail = gk[:, :mid], gk[:, mid:]
        grad_q_lat = grad_q_lat.astype(BF16)
        grad_kv_all = jnp.concatenate([grad_kv_lat, gk_lead * cos_here + gk_tail * sin_here, gk_tail * cos_here - gk_lead * sin_here], axis=1).astype(BF16)
        own = dim // shards
        own_kv = kv_width // shards * dim // q_rank
        part_dq = dot(normed, grad_q_lat, 0, 0).astype(BF16).reshape(shards, own, q_rank)
        part_dkv = dot(grad_kv_all, normed, 0, 0).astype(BF16).reshape(shards, own_kv, q_rank)
        down_part, dk_all, dv_all = lax.optimization_barrier((jnp.concatenate([part_dq, part_dkv], axis=1), dk_all, dv_all))
        down_sum = lax.psum_scatter(down_part, 'tp', scatter_dimension=0, tiled=False)
        gwk, gwv = weight_grads(q_rank, kv_rank, [dk_all, dv_all])
        grad_w_uk = gwk.reshape(heads, nope, kv_rank).transpose(2, 0, 1)
        grad_w_uv = gwv.reshape(heads, value, kv_rank).transpose(2, 0, 1)
        grad_normed = dot(grad_q_lat, w_dq, 1, 1) + dot(grad_kv_all, w_dkv, 1, 1)
        grad_x_norm, grad_norm_gain = norm_backward(grad_normed, x_unit, x_inv, norm_gain)
        grad_hidden = grad_out.reshape(here, dim).astype(F32) + grad_x_norm

        gains = jnp.concatenate([grad_norm_gain, grad_q_gain, grad_kv_gain])
        gain_rows = -(-gains.shape[0] // q_rank)
        gains = jnp.pad(gains, (0, gain_rows * q_rank - gains.shape[0])).reshape(gain_rows, q_rank)
        high = lax.reduce_precision(gains, 8, 7)
        middle = lax.reduce_precision(gains - high, 8, 7)
        tail = gains - high - middle
        packed = jnp.concatenate([down_sum, high.astype(BF16), middle.astype(BF16), tail.astype(BF16)], axis=0)
        gathered = lax.all_gather(packed, 'tp', axis=0)
        grad_w_dq = gathered[:, :own].reshape(dim, q_rank).astype(F32)
        grad_w_dkv = gathered[:, own:own + own_kv].reshape(kv_width, dim).astype(F32).T
        terms = gathered[:, own + own_kv:].astype(F32).reshape(shards, 3, gain_rows * q_rank)
        sums = jnp.sum(terms[:, 0] + terms[:, 1] + terms[:, 2], axis=0)
        g_norm = sums[:dim]
        g_q = sums[dim:dim + q_rank]
        g_kv = sums[dim + q_rank:dim + q_rank + kv_rank]
        return (out_hidden, grad_hidden.reshape(batch, rows, dim), g_norm, grad_w_dq, g_q, grad_w_dkv, g_kv, grad_w_uq, grad_w_qr, grad_w_uk, grad_w_uv, grad_w_out)

    return jax.shard_map(local_step, mesh=mesh, in_specs=in_specs, out_specs=out_specs, check_vma=False)
```
